32 devices in a mesh: seq: 8 (over y, x, core), tensor: 4 (over z).
Axes of the slice: x: 2, y: 2, z: 4, core: 2. Of those that a mesh axis runs over, the one named last changes fastest.
Arguments:
- tokens: bfloat16 [4096, 8192], P('seq', 'tensor'), may hold values from -6 to 6
- positions: int32 [4096], P('seq'), may hold values from 0 to 4095, each once
- norm_gain: float32 [8192], replicated, may hold values from 0.1 to 1.9
- w_query: bfloat16 [8192, 4096], P('seq', 'tensor'), may hold values from -0.0625 to 0.0625
- w_key: bfloat16 [8192, 1024], P('seq', 'tensor'), may hold values from -0.0625 to 0.0625
- w_value: bfloat16 [8192, 1024], P('seq', 'tensor'), may hold values from -0.0625 to 0.0625
- b_query: float32 [4096], P('tensor'), may hold values from -40 to 40
- b_key: float32 [1024], P('tensor'), may hold values from -40 to 40
- b_value: float32 [1024], P('tensor'), may hold values from -6 to 6
- w_out: bfloat16 [4096, 8192], P('tensor', 'seq'), may hold values from -0.09375 to 0.09375
Outputs:
- mixed: bfloat16 [4096, 8192], P('seq', 'tensor')
- context: bfloat16 [4096, 4096], P('seq', 'tensor')
The draws below stay inside these ranges and needn't reach their ends.
Inputs may be any that keep to these rules, and one draw needn't show every extreme that they name: positions holds every position 0 to 4095 once.
All inputs are finite; a program needn't handle non-finite values.
Results may differ from the reference program's by a relative error of at most 0.025.
Values may be sent and summed in bfloat16 or wider, within the bound.
A program may use at most 128 MiB of HBM per device.

```python
import jax
import jax.numpy as jnp
from jax import lax

D = 8192
HEADS = 32
KV_HEADS = 8
HD = 128
TOKENS = 4096


def draw_b_query(key, part):
    return jax.random.normal(jax.random.fold_in(key, 14), (HEADS * HD,), jnp.float32)


def draw_b_key(key, part):
    return jax.random.normal(jax.random.fold_in(key, 15), (KV_HEADS * HD,), jnp.float32)


def steps_of(rng, dims, cuts, low, high):
    factor_of, own = 1.0, jax.random.fold_in(rng, 6)
    for position, parts in cuts:
        steps = jnp.exp(jax.random.uniform(jax.random.fold_in(own, position), (parts,), jnp.float32, low / len(cuts), high / len(cuts)))
        factor_of = factor_of * jnp.repeat(steps, dims[position] // parts).reshape([-1 if axis == position else 1 for axis in range(len(dims))])
    return factor_of


def centred(own_key, dims, deviation, bound, split=(), held_as=jnp.bfloat16):
    loudness = steps_of(own_key, dims, split, -0.22, 0.18) if split else 1.0
    array = jax.random.normal(own_key, dims, jnp.float32) * deviation * loudness
    return jnp.minimum(jnp.maximum(array, -bound), bound).astype(held_as)


def setup_inputs(seed: int = 0) -> dict:
    splits = jax.random.split(jax.random.key(seed), 11)
    tokens = centred(splits[0], (TOKENS, D), 1.0, 6.0, ((0, 8), (1, 4)))
    positions = jax.random.permutation(splits[1], TOKENS).astype(jnp.int32)
    norm_gain = jnp.clip(1.0 + 0.18 * jax.random.normal(splits[2], (D,), jnp.float32), 0.1, 1.9)
    w_query = centred(splits[3], (D, HEADS * HD), D ** -0.5, 0.0625, ((0, 8), (1, 4)))
    w_key = centred(splits[4], (D, KV_HEADS * HD), D ** -0.5, 0.0625, ((0, 8), (1, 4)))
    w_value = centred(splits[5], (D, KV_HEADS * HD), D ** -0.5, 0.0625, ((0, 8), (1, 4)))
    b_query = draw_b_query(jax.random.fold_in(splits[10], 71), 0)
    b_key = draw_b_key(jax.random.fold_in(splits[10], 71), 0)
    b_value = centred(splits[8], (KV_HEADS * HD,), 1.0, 6.0, ((0, 4),), jnp.float32)
    w_out = centred(splits[9], (HEADS * HD, D), (HEADS * HD) ** -0.5, 0.09375, ((0, 4), (1, 8)))
    return dict(tokens=tokens, positions=positions, norm_gain=norm_gain, w_query=w_query, w_key=w_key, w_value=w_value, b_query=b_query, b_key=b_key, b_value=b_value, w_out=w_out)


NORM_EPS = 1e-06
ROPE_BASE = 1000000.0
NEG_FILL = -1e+30

def rotate(values_in, positions):
    half_dim = HD // 2
    inv_freq = ROPE_BASE ** (-jnp.arange(half_dim, dtype=jnp.float32) * 2.0 / HD)
    angles = positions.astype(jnp.float32)[:, None] * inv_freq[None, :]
    cosine = jnp.cos(angles)[:, None, :]
    sines = jnp.sin(angles)[:, None, :]
    lower_half = values_in[..., :half_dim]
    upper_half = values_in[..., half_dim:]
    return jnp.concatenate([lower_half * cosine - upper_half * sines, upper_half * cosine + lower_half * sines], -1)

def reference(tokens, positions, norm_gain, w_query, w_key, w_value, b_query, b_key, b_value, w_out):
    group = HEADS // KV_HEADS
    inputs = tokens.astype(jnp.float32)
    inverse_rms = lax.rsqrt(lax.optimization_barrier(jnp.mean(inputs * inputs, -1, keepdims=True)) + NORM_EPS)
    normed = (inputs * inverse_rms * norm_gain.astype(jnp.float32)[None, :]).astype(jnp.bfloat16)
    q_proj = jnp.dot(normed, w_query, preferred_element_type=jnp.float32) + b_query.astype(jnp.float32)[None, :]
    k_proj = jnp.dot(normed, w_key, preferred_element_type=jnp.float32) + b_key.astype(jnp.float32)[None, :]
    v_proj = jnp.dot(normed, w_value, preferred_element_type=jnp.float32) + b_value.astype(jnp.float32)[None, :]
    queries = rotate(q_proj.reshape(TOKENS, HEADS, HD), positions).astype(jnp.bfloat16)
    keys_rot = rotate(k_proj.reshape(TOKENS, KV_HEADS, HD), positions).astype(jnp.bfloat16)
    values = v_proj.astype(jnp.bfloat16).reshape(TOKENS, KV_HEADS, HD)
    queries = jnp.moveaxis(queries, 1, 0)
    keys_rot = jnp.moveaxis(keys_rot, 1, 0)
    values = jnp.moveaxis(values, 1, 0)
    allowed = positions[None, :] <= positions[:, None]
    scale = HD ** (-0.5)

    def one_head(head_index):
        q_head = lax.dynamic_index_in_dim(queries, head_index, 0, keepdims=False).astype(jnp.float32)
        kv_index = head_index // group
        k_head = lax.dynamic_index_in_dim(keys_rot, kv_index, 0, keepdims=False).astype(jnp.float32)
        v_head = lax.dynamic_index_in_dim(values, kv_index, 0, keepdims=False)
        scores = jnp.dot(q_head, k_head.T) * scale
        scores = jnp.where(allowed, scores, NEG_FILL)
        row_max = lax.optimization_barrier(jnp.max(scores, -1, keepdims=True))
        weights = jnp.where(allowed, jnp.exp(scores - row_max), 0.0)
        denominator = lax.optimization_barrier(jnp.sum(weights, -1, keepdims=True))
        numerator = jnp.dot(weights.astype(jnp.bfloat16), v_head, preferred_element_type=jnp.float32)
        return (numerator / denominator).astype(jnp.bfloat16)
    per_head = lax.map(one_head, jnp.arange(HEADS, dtype=jnp.int32))
    context = jnp.moveaxis(per_head, 0, 1).reshape(TOKENS, HEADS * HD)
    mixed = (inputs + jnp.dot(context, w_out, preferred_element_type=jnp.float32)).astype(jnp.bfloat16)
    return (mixed, context)
```

```python
import functools

import jax
import jax.numpy as jnp
from jax import lax
from jax.experimental import pallas as pl
from jax.experimental.pallas import tpu as pltpu
from jax.sharding import PartitionSpec as P

HD = 128


NORM_EPS = 1e-06
ROPE_BASE = 1000000.0
NEG_FILL = -1e30
CORES = 2
PAIR = 2
PLANE_SEMS = 10
MESH = pl.DeviceIdType.MESH
ANY = pl.BlockSpec(memory_space=pl.ANY)
VMEM = pl.BlockSpec(memory_space=pltpu.VMEM)


def plane_sems(n):
    chips = n // CORES
    return PLANE_SEMS if chips == 4 else 2 * chips


def plane_partners(n, s):
    twin = s + 1 - 2 * (s % CORES)
    chips = n // CORES
    if chips == 4:
        return [twin, s + 2 - 4 * ((s // 2) % 2), (s + 4) % n]
    return [twin] + [(s + CORES * j) % n for j in range(1, chips)]


def plane_gather(n, s, items, send_sem, recv_sem):
    twin = s + 1 - 2 * (s % CORES)
    chips = n // CORES

    def copy(item, sem, source, dest, target):
        return pltpu.make_async_remote_copy(
            src_ref=source,
            dst_ref=dest,
            send_sem=send_sem.at[item, sem],
            recv_sem=recv_sem.at[item, sem],
            device_id={"seq": target},
            device_id_type=MESH,
        )

    if chips == 4:
        xn = s + 2 - 4 * ((s // 2) % 2)
        yn = (s + 4) % n
        dg = (xn + 4) % n

        def half(ref, item, i):
            rows = items[item][2] // 2
            return ref.at[pl.ds(i * rows, rows), :]

        def piece(item, sem, block, i, target, own=False):
            source, slot, _ = items[item]
            dest = half(slot(block), item, i)
            return copy(item, sem, half(source, item, i) if own else dest, dest, target)

        def across(item, sem, block, own=False):
            source, slot, _ = items[item]
            return copy(item, sem, source if own else slot(block), slot(block), twin)

        def other(block):
            return block + 1 - 2 * (block % CORES)

        def start(item):
            piece(item, 0, s, 0, xn, True).start()
            piece(item, 3, s, 1, yn, True).start()
            piece(item, 1, s, 1, xn, True).start()
            piece(item, 2, s, 0, yn, True).start()
            across(item, 6, s, True).start()

        def relay(item, stage):
            if stage == 0:
                piece(item, 0, xn, 0, xn).wait_recv()
                piece(item, 4, xn, 0, yn).start()
                piece(item, 3, yn, 1, yn).wait_recv()
                piece(item, 5, yn, 1, xn).start()
            elif stage == 1:
                piece(item, 1, xn, 1, xn).wait_recv()
                across(item, 7, xn).start()
                piece(item, 2, yn, 0, yn).wait_recv()
                across(item, 8, yn).start()
            else:
                piece(item, 4, dg, 0, yn).wait_recv()
                piece(item, 5, dg, 1, xn).wait_recv()
                across(item, 9, dg).start()

        def finish(item):
            for sem, block in ((6, s), (7, xn), (8, yn), (9, dg)):
                across(item, sem, other(block)).wait_recv()

        def drain(item):
            piece(item, 0, s, 0, xn, True).wait_send()
            piece(item, 3, s, 1, yn, True).wait_send()
            piece(item, 1, s, 1, xn, True).wait_send()
            piece(item, 2, s, 0, yn, True).wait_send()
            piece(item, 4, xn, 0, yn).wait_send()
            piece(item, 5, yn, 1, xn).wait_send()
            across(item, 6, s, True).wait_send()
            for sem, block in ((7, xn), (8, yn), (9, dg)):
                across(item, sem, block).wait_send()

    else:

        def hop(item, kind, j, block, own, target):
            source, slot, _ = items[item]
            return copy(item, kind * chips + j, source if own else slot(block), slot(block), target)

        def start(item):
            for j in range(1, chips):
                hop(item, 0, j, s, True, (s + CORES * j) % n).start()
            hop(item, 1, 0, s, True, twin).start()

        def relay(item, stage):
            if stage == 2:
                for j in range(1, chips):
                    origin = (s + n - CORES * j) % n
                    hop(item, 0, j, origin, False, origin).wait_recv()
                    hop(item, 1, j, origin, False, twin).start()

        def finish(item):
            for j in range(chips):
                hop(item, 1, j, (twin + n - CORES * j) % n, False, twin).wait_recv()

        def drain(item):
            for j in range(1, chips):
                hop(item, 0, j, s, True, (s + CORES * j) % n).wait_send()
            hop(item, 1, 0, s, True, twin).wait_send()
            for j in range(1, chips):
                hop(item, 1, j, (s + n - CORES * j) % n, False, twin).wait_send()

    return start, relay, finish, drain


def line_sends(m, t, step):
    right = (t >= step) & (t < m - 1)
    left = (t + step < m) & (t > 0)
    return (right, 0, t - step, t + 1), (left, 1, t + step, t - 1)


def line_takes(m, t, step):
    return (
        (t - 1 - step >= 0, 0, t - 1 - step, t - 1),
        (t + 1 + step < m, 1, t + 1 + step, t + 1),
    )


def line_neighbours(m, t, act):
    @pl.when(t > 0)
    def _():
        act(t - 1)

    @pl.when(t < m - 1)
    def _():
        act(t + 1)


def project_kernel(
    n, m, tokens, w_query, w_key, w_value, w_out, gain, bias, cosine, sine, q, kv, w_mix,
    tok_all, wq_all, wkv_all, acc, squares, scaled,
    plane_send, plane_recv, line_send, line_recv, mix_send, mix_recv, local_sem,
):
    s = lax.axis_index("seq")
    t = lax.axis_index("tensor")
    heads, rows, _ = q.shape
    kv_heads = kv.shape[0]
    depth, query_cols = w_query.shape
    key_cols = w_key.shape[1]
    feats = tokens.shape[1]
    g = n // m
    part = s % g
    home = s // g
    piece_rows = w_out.shape[0] // m

    barrier = pltpu.get_barrier_semaphore()
    partners = plane_partners(n, s)
    for other in partners:
        pl.semaphore_signal(barrier, inc=1, device_id={"seq": other}, device_id_type=MESH)
    line_neighbours(
        m, t, lambda o: pl.semaphore_signal(barrier, inc=1, device_id={"tensor": o}, device_id_type=MESH)
    )
    for p in range(m):

        @pl.when(home != p)
        def _():
            pl.semaphore_signal(barrier, inc=1, device_id={"seq": g * p + part}, device_id_type=MESH)

    ends = jnp.where(t > 0, 1, 0) + jnp.where(t < m - 1, 1, 0)
    pl.semaphore_wait(barrier, len(partners) + ends + (m - 1))

    def wq_slot(b):
        return wq_all.at[pl.ds(pl.multiple_of(b * depth, 128), depth), :]

    def wk_slot(b):
        return wkv_all.at[pl.ds(pl.multiple_of(b * depth, 128), depth), pl.ds(0, key_cols)]

    def wv_slot(b):
        return wkv_all.at[pl.ds(pl.multiple_of(b * depth, 128), depth), pl.ds(key_cols, key_cols)]

    items = [(w_query, wq_slot, depth), (w_key, wk_slot, depth), (w_value, wv_slot, depth)]
    start, relay, finish, drain = plane_gather(n, s, items, plane_send, plane_recv)

    def line(way, step, block, first, target):
        return pltpu.make_async_remote_copy(
            src_ref=tokens if first else tok_all.at[block],
            dst_ref=tok_all.at[block],
            send_sem=line_send.at[way, step],
            recv_sem=line_recv.at[way, step],
            device_id={"tensor": target},
            device_id_type=MESH,
        )

    def send_line(step):
        for cond, way, block, target in line_sends(m, t, step):

            @pl.when(cond)
            def _():
                line(way, step, block, step == 0, target).start()

    def take_line(step):
        for valid, way, block, source in line_takes(m, t, step):

            @pl.when(valid)
            def _():
                line(way, step, block, False, source).wait_recv()

    send_line(0)
    for item in range(3):
        start(item)

    def mix(p):
        return pltpu.make_async_remote_copy(
            src_ref=w_out.at[pl.ds(p * piece_rows, piece_rows), :],
            dst_ref=w_mix.at[home],
            send_sem=mix_send.at[p],
            recv_sem=mix_recv.at[home],
            device_id={"seq": g * p + part},
            device_id_type=MESH,
        )

    def mixed_in(f):
        return pltpu.make_async_remote_copy(
            src_ref=w_mix.at[f],
            dst_ref=w_mix.at[f],
            send_sem=mix_send.at[f],
            recv_sem=mix_recv.at[f],
            device_id={"seq": g * f + part},
            device_id_type=MESH,
        )

    own = [
        pltpu.make_async_copy(tokens, tok_all.at[t], local_sem.at[0]),
        pltpu.make_async_copy(w_query, wq_slot(s), local_sem.at[1]),
        pltpu.make_async_copy(w_key, wk_slot(s), local_sem.at[2]),
        pltpu.make_async_copy(w_value, wv_slot(s), local_sem.at[3]),
    ]
    for copy in own:
        copy.start()
    acc[...] = jnp.zeros_like(acc)
    squares[...] = jnp.zeros_like(squares)

    for item in range(3):
        relay(item, 0)
    for p in range(m):

        @pl.when(home != p)
        def _():
            mix(p).start()

    step_of = 0
    for stage in (1, 2):
        if step_of < m - 1:
            take_line(step_of)
            step_of += 1
            if step_of < m - 1:
                send_line(step_of)
        for item in range(3):
            relay(item, stage)
    while step_of < m - 2:
        take_line(step_of)
        step_of += 1
        send_line(step_of)
    for copy in own:
        copy.wait()
    for item in range(3):
        finish(item)

    part_feats = depth
    parts = feats // part_feats

    def multiply(block):
        def one(i, _):
            at = pl.multiple_of(i * part_feats, 128)
            x = tok_all[block, :, pl.ds(at, part_feats)].astype(jnp.float32)
            sq = x * x
            total = sq[:, 0:128]
            for c in range(1, part_feats // 128):
                total = total + sq[:, c * 128 : (c + 1) * 128]
            squares[...] += total
            scaled[...] = (x * gain[block, :, pl.ds(at, part_feats)]).astype(jnp.bfloat16)
            row = pl.multiple_of(block * feats + at, 128)
            half = query_cols // 2
            for c in range(2):
                cols = slice(c * half, (c + 1) * half)
                acc[:, cols] += jnp.dot(
                    scaled[...], wq_all[pl.ds(row, part_feats), cols], preferred_element_type=jnp.float32
                )
            acc[:, query_cols:] += jnp.dot(
                scaled[...], wkv_all[pl.ds(row, part_feats), :], preferred_element_type=jnp.float32
            )
            return 0

        lax.fori_loop(0, parts, one, 0)

    multiply(t)
    for step in range(m - 1):
        if step == m - 2:
            take_line(step)
        for valid, _, block, _ in line_takes(m, t, step):

            @pl.when(valid)
            def _():
                multiply(block)

    mean = jnp.sum(squares[...], -1, keepdims=True) / (m * feats)
    inverse_rms = lax.rsqrt(mean + NORM_EPS)

    def head(i):
        cols = slice(i * HD, (i + 1) * HD)
        return acc[:, cols] * inverse_rms + bias[:, cols]

    def turned(i):
        value = head(i)
        return (value * cosine[...] + pltpu.roll(value, HD // 2, 1) * sine[...]).astype(jnp.bfloat16)

    for h in range(heads):
        q[h] = turned(h)
    for h in range(kv_heads):
        kv[h, :, 0:HD] = turned(heads + h)
        kv[h, :, HD : 2 * HD] = head(heads + kv_heads + h).astype(jnp.bfloat16)

    for item in range(3):
        drain(item)
    for p in range(m):

        @pl.when(home != p)
        def _():
            mix(p).wait_send()
            mixed_in(p).wait_recv()

    for step in range(m - 1):
        for cond, way, block, target in line_sends(m, t, step):

            @pl.when(cond)
            def _():
                line(way, step, block, step == 0, target).wait_send()


def project(n, m, tokens, w_query, w_key, w_value, w_out, gain, bias, cosine, sine):
    rows, feats = tokens.shape
    depth, query_cols = w_query.shape
    key_cols = w_key.shape[1]
    heads, kv_heads = query_cols // HD, key_cols // HD
    wrows, wcols = w_out.shape
    bf16, f32 = jnp.bfloat16, jnp.float32
    dma = pltpu.SemaphoreType.DMA
    return pl.pallas_call(
        functools.partial(project_kernel, n, m),
        out_shape=(
            jax.ShapeDtypeStruct((heads, rows, HD), bf16),
            jax.ShapeDtypeStruct((kv_heads, rows, 2 * HD), bf16),
            jax.ShapeDtypeStruct((m, wrows // m, wcols), bf16),
        ),
        in_specs=[ANY] * 5 + [VMEM] * 4,
        out_specs=(VMEM, VMEM, ANY),
        scratch_shapes=[
            pltpu.VMEM((m, rows, feats), bf16),
            pltpu.VMEM((n * depth, query_cols), bf16),
            pltpu.VMEM((n * depth, 2 * key_cols), bf16),
            pltpu.VMEM((rows, query_cols + 2 * key_cols), f32),
            pltpu.VMEM((rows, 128), f32),
            pltpu.VMEM((rows, depth), bf16),
            dma((3, plane_sems(n))),
            dma((3, plane_sems(n))),
            dma((2, m - 1)),
            dma((2, m - 1)),
            dma((m,)),
            dma((m,)),
            dma((4,)),
        ],
        compiler_params=pltpu.CompilerParams(
            collective_id=0, has_side_effects=True, vmem_limit_bytes=60 * 2**20
        ),
        cost_estimate=pl.CostEstimate(flops=10**11, bytes_accessed=10**8, transcendentals=0),
    )(tokens, w_query, w_key, w_value, w_out, gain, bias, cosine, sine)


def attend_kernel(
    n, m, q, kv, pos, qpos, tokens, w_out, w_mix, mixed, context,
    kv_all, pos_all, ctx_all, w_all, scores, biggest, total, acc, residual,
    plane_send, plane_recv, swap_send, swap_recv, line_send, line_recv, local_sem,
):
    s = lax.axis_index("seq")
    t = lax.axis_index("tensor")
    heads, rows, _ = q.shape
    kv_heads = kv.shape[0]
    group = heads // kv_heads
    g = n // m
    part = s % g
    home = s // g
    wrows, wcols = w_out.shape
    piece_rows = wrows // m
    chunks = heads // PAIR
    width = PAIR * HD
    outs = acc.shape[1]

    barrier = pltpu.get_barrier_semaphore()
    partners = plane_partners(n, s)
    for other in partners:
        pl.semaphore_signal(barrier, inc=1, device_id={"seq": other}, device_id_type=MESH)
    for other in range(m):

        @pl.when(t != other)
        def _():
            pl.semaphore_signal(barrier, inc=1, device_id={"tensor": other}, device_id_type=MESH)

    pl.semaphore_wait(barrier, len(partners) + m - 1)

    def kv_slot(h):
        return lambda b: kv_all.at[h, pl.ds(pl.multiple_of(b * rows, 128), rows), :]

    def w_slot(b, tt):
        return w_all.at[
            pl.ds(pl.multiple_of(tt * wrows + (b // g) * piece_rows, 16), piece_rows),
            pl.ds(pl.multiple_of((b % g) * wcols, 128), wcols),
        ]

    items = [(kv.at[h], kv_slot(h), rows) for h in range(kv_heads)]
    items.append((pos, lambda b: pos_all.at[b], pos.shape[0]))
    first_w = len(items)
    turn = 1 - 2 * (t // (m // 2))
    order = [(t + m + d * turn) % m for d in range(m)]
    for tt in order:
        items.append((w_slot(s, tt), lambda b, tt=tt: w_slot(b, tt), piece_rows))
    start, relay, finish, drain = plane_gather(n, s, items, plane_send, plane_recv)

    start(first_w - 1)
    for h in range(kv_heads):
        start(h)

    def swap(f, own):
        source = w_out.at[pl.ds(pl.multiple_of(home * piece_rows, 16), piece_rows), :]
        return pltpu.make_async_remote_copy(
            src_ref=source if own else w_mix.at[f],
            dst_ref=w_slot(s, t),
            send_sem=swap_send.at[f],
            recv_sem=swap_recv.at[t],
            device_id={"tensor": f},
            device_id_type=MESH,
        )

    def keep(own):
        source = w_out.at[pl.ds(pl.multiple_of(home * piece_rows, 16), piece_rows), :]
        return pltpu.make_async_copy(source if own else w_mix.at[t], w_slot(s, t), local_sem.at[0])

    for f in order[1:]:

        @pl.when(home == f)
        def _():
            swap(f, True).start()

        @pl.when(home != f)
        def _():
            swap(f, False).start()

    @pl.when(home == t)
    def _():
        keep(True).start()

    @pl.when(home != t)
    def _():
        keep(False).start()

    for h in range(kv_heads):
        kv_all[h, pl.ds(pl.multiple_of(s * rows, 128), rows), :] = kv[h]
    pos_all[s] = pos[...]

    load = pltpu.make_async_copy(tokens, residual, local_sem.at[1])
    load.start()

    def arrived(tt):
        pltpu.make_async_remote_copy(
            src_ref=w_slot(s, tt),
            dst_ref=w_slot(s, tt),
            send_sem=swap_send.at[tt],
            recv_sem=swap_recv.at[tt],
            device_id={"tensor": tt},
            device_id_type=MESH,
        ).wait_recv()

    def line(way, step, chunk, block, target):
        return pltpu.make_async_remote_copy(
            src_ref=ctx_all.at[block, chunk],
            dst_ref=ctx_all.at[block, chunk],
            send_sem=line_send.at[way, step, chunk],
            recv_sem=line_recv.at[way, step, chunk],
            device_id={"tensor": target},
            device_id_type=MESH,
        )

    def send_line(step, chunk):
        for cond, way, block, target in line_sends(m, t, step):

            @pl.when(cond)
            def _():
                line(way, step, chunk, block, target).start()

    query_pos = qpos[...]
    scale = HD ** (-0.5) * 1.4426950408889634

    def attend(h):
        base = h // group

        def block_scores(b, _):
            at = pl.multiple_of(b * rows, 128)
            keys = kv_all[base, pl.ds(at, rows), 0:HD]
            raw = lax.dot_general(
                q[h], keys, (((1,), (1,)), ((), ())), preferred_element_type=jnp.float32
            )
            masked = jnp.where(pos_all[b, 0:1, :] <= query_pos, raw, NEG_FILL)
            scores[b] = masked
            top = biggest[...]
            for i in range(rows // 128):
                top = jnp.maximum(top, masked[:, i * 128 : (i + 1) * 128])
            biggest[...] = top
            return 0

        biggest[...] = jnp.full_like(biggest, NEG_FILL)
        lax.fori_loop(0, n, block_scores, 0)
        row_max = jnp.max(biggest[...], -1, keepdims=True) * scale
        total[...] = jnp.zeros_like(total)
        biggest[...] = jnp.zeros_like(biggest)

        def block_values(b, _):
            at = pl.multiple_of(b * rows, 128)
            weights = jnp.exp2(scores[b] * scale - row_max)
            value = kv_all[base, pl.ds(at, rows), HD : 2 * HD]
            total[...] += jnp.dot(
                weights.astype(jnp.bfloat16), value, preferred_element_type=jnp.float32
            )
            add = weights[:, 0:128]
            for i in range(1, rows // 128):
                add = add + weights[:, i * 128 : (i + 1) * 128]
            biggest[...] += add
            return 0

        lax.fori_loop(0, n, block_values, 0)
        denominator = jnp.sum(biggest[...], -1, keepdims=True)
        return (total[...] / denominator).astype(jnp.bfloat16)

    for stage in range(3):
        relay(first_w - 1, stage)
        for h in range(kv_heads):
            relay(h, stage)
    keep(True).wait()
    start(first_w)
    finish(first_w - 1)

    work = []
    for d in range(1, m):
        work.append([("start", d), ("relay", d - 1, 0)])
        if d > 1:
            work[-1].append(("relay", d - 2, 1))
        if d > 2:
            work[-1].append(("relay", d - 3, 2))

    def advance(jobs):
        for job in jobs:
            if job[0] == "start":
                arrived(order[job[1]])
                start(first_w + job[1])
            else:
                relay(first_w + job[1], job[2])

    rest = []
    for d in range(m):
        for stage in range(3):
            if all(("relay", d, stage) not in jobs for jobs in work):
                rest.append((d + stage, d, ("relay", d, stage)))
    rest = [job for _, _, job in sorted(rest)]

    stored = []
    for chunk in range(chunks):
        base = chunk * PAIR // group
        if chunk * PAIR % group == 0:
            finish(base)

        def one(i, _):
            value = attend(chunk * PAIR + i)
            ctx_all[t, chunk, :, pl.ds(pl.multiple_of(i * HD, HD), HD)] = value
            return 0

        lax.fori_loop(0, PAIR, one, 0)
        send_line(0, chunk)
        out = pltpu.make_async_copy(
            ctx_all.at[t, chunk],
            context.at[:, pl.ds(chunk * width, width)],
            local_sem.at[2 + chunk],
        )
        out.start()
        stored.append(out)
        if chunk < len(work):
            advance(work[chunk])
    for jobs in work[chunks:]:
        advance(jobs)

    load.wait()

    def out_proj(block, first):
        for j in range(outs // wcols):
            cols = slice(j * wcols, (j + 1) * wcols)

            def partial(c):
                at = pl.multiple_of(block * wrows + c * width, 128)
                return jnp.dot(
                    ctx_all[block, c], w_all[pl.ds(at, width), cols], preferred_element_type=jnp.float32
                )

            value = partial(0)
            for c in range(1, chunks):
                value = value + partial(c)
            acc[:, cols] = value + (residual[:, cols].astype(jnp.float32) if first else acc[:, cols])

    def take_line(step):
        for valid, way, block, source in line_takes(m, t, step):
            for chunk in range(chunks):

                @pl.when(valid)
                def _():
                    line(way, step, chunk, block, source).wait_recv()

                if step + 1 < m - 1:
                    go = valid & ((t < m - 1) if way == 0 else (t > 0))
                    onward = t + 1 if way == 0 else t - 1

                    @pl.when(go)
                    def _():
                        line(way, step + 1, chunk, block, onward).start()

    def add_blocks(step):
        def way(i, _):
            block = jnp.where(i == 0, t - 1 - step, t + 1 + step)

            @pl.when((block >= 0) & (block < m))
            def _():
                out_proj(block, False)

            return 0

        lax.fori_loop(0, 2, way, 0)

    take_line(0)
    cut = (len(rest) + 1) // 2
    advance(rest[:cut])
    for step in range(1, m - 2):
        take_line(step)
    advance(rest[cut:])
    for d in range(m):
        finish(first_w + d)
    out_proj(t, True)
    for step in range(m - 1):
        if step == m - 2 and step > 0:
            take_line(step)
        add_blocks(step)

    residual[...] = acc[...].astype(jnp.bfloat16)
    final = pltpu.make_async_copy(residual, mixed, local_sem.at[1])
    final.start()

    for item in range(len(items)):
        drain(item)
    for f in order[1:]:
        swap(f, False).wait_send()

    for step in range(m - 1):
        for cond, way, block, target in line_sends(m, t, step):
            for chunk in range(chunks):

                @pl.when(cond)
                def _():
                    line(way, step, chunk, block, target).wait_send()

    for out in stored:
        out.wait()
    final.wait()


def attend_and_mix(n, m, q, kv, pos, qpos, tokens, w_out, w_mix):
    heads, rows, _ = q.shape
    kv_heads = kv.shape[0]
    wrows, wcols = w_out.shape
    outs = tokens.shape[1]
    chunks = heads // PAIR
    items = kv_heads + 1 + m
    bf16, f32 = jnp.bfloat16, jnp.float32
    dma = pltpu.SemaphoreType.DMA
    return pl.pallas_call(
        functools.partial(attend_kernel, n, m),
        out_shape=(
            jax.ShapeDtypeStruct(tokens.shape, bf16),
            jax.ShapeDtypeStruct((rows, heads * HD), bf16),
        ),
        in_specs=[VMEM, VMEM, VMEM, VMEM, ANY, ANY, ANY],
        out_specs=(ANY, ANY),
        scratch_shapes=[
            pltpu.VMEM((kv_heads, n * rows, 2 * HD), bf16),
            pltpu.VMEM((n, *pos.shape), pos.dtype),
            pltpu.VMEM((m, chunks, rows, PAIR * HD), bf16),
            pltpu.VMEM((m * wrows, outs), bf16),
            pltpu.VMEM((n, rows, rows), f32),
            pltpu.VMEM((rows, 128), f32),
            pltpu.VMEM((rows, HD), f32),
            pltpu.VMEM((rows, outs), f32),
            pltpu.VMEM((rows, outs), bf16),
            dma((items, plane_sems(n))),
            dma((items, plane_sems(n))),
            dma((m,)),
            dma((m,)),
            dma((2, m - 1, chunks)),
            dma((2, m - 1, chunks)),
            dma((2 + chunks,)),
        ],
        compiler_params=pltpu.CompilerParams(
            collective_id=1, has_side_effects=True, vmem_limit_bytes=60 * 2**20
        ),
        cost_estimate=pl.CostEstimate(flops=10**11, bytes_accessed=10**8, transcendentals=0),
    )(q, kv, pos, qpos, tokens, w_out, w_mix)


def shards(seq, tensor, tokens, positions, norm_gain, w_query, w_key, w_value, b_query, b_key, b_value, w_out):
    rows, feats = tokens.shape
    half = HD // 2
    inv_freq = ROPE_BASE ** (-jnp.arange(half, dtype=jnp.float32) * 2.0 / HD)
    inv_freq = jnp.concatenate((inv_freq, inv_freq))
    sign = jnp.where(jnp.arange(HD) < half, -1.0, 1.0)
    angles = positions.astype(jnp.float32)[:, None] * inv_freq[None, :]
    cosine = jnp.cos(angles)
    sine = jnp.sin(angles) * sign[None, :]
    bias = jnp.concatenate((b_query, b_key, b_value))[None, :]
    pos = jnp.broadcast_to(positions[None, :], (16, rows))
    q, kv, w_mix = project(
        seq, tensor, tokens, w_query, w_key, w_value, w_out,
        norm_gain.reshape(tensor, 1, feats), bias, cosine, sine,
    )
    return attend_and_mix(seq, tensor, q, kv, pos, positions[:, None], tokens, w_out, w_mix)


def solution(mesh):
    in_specs = (
        P("seq", "tensor"),
        P("seq"),
        P(),
        P("seq", "tensor"),
        P("seq", "tensor"),
        P("seq", "tensor"),
        P("tensor"),
        P("tensor"),
        P("tensor"),
        P("tensor", "seq"),
    )
    out_specs = (P("seq", "tensor"), P("seq", "tensor"))

    def body(*args):
        return shards(mesh.shape["seq"], mesh.shape["tensor"], *args)

    return jax.shard_map(body, mesh=mesh, in_specs=in_specs, out_specs=out_specs, check_vma=False)
```

```python
import functools

import jax
import jax.numpy as jnp
from jax import lax
from jax.experimental import pallas as pl
from jax.experimental.pallas import tpu as pltpu
from jax.sharding import PartitionSpec as P

HD = 128


NORM_EPS = 1e-06
ROPE_BASE = 1000000.0
NEG_FILL = -1e30
CORES = 2
PAIR = 2
PLANE_SEMS = 10
MESH = pl.DeviceIdType.MESH
ANY = pl.BlockSpec(memory_space=pl.ANY)
VMEM = pl.BlockSpec(memory_space=pltpu.VMEM)


def plane_sems(n):
    chips = n // CORES
    return PLANE_SEMS if chips == 4 else 2 * chips


def plane_partners(n, s):
    twin = s + 1 - 2 * (s % CORES)
    chips = n // CORES
    if chips == 4:
        return [twin, s + 2 - 4 * ((s // 2) % 2), (s + 4) % n]
    return [twin] + [(s + CORES * j) % n for j in range(1, chips)]


def plane_gather(n, s, items, send_sem, recv_sem):
    twin = s + 1 - 2 * (s % CORES)
    chips = n // CORES

    def copy(item, sem, source, dest, target):
        return pltpu.make_async_remote_copy(
            src_ref=source,
            dst_ref=dest,
            send_sem=send_sem.at[item, sem],
            recv_sem=recv_sem.at[item, sem],
            device_id={"seq": target},
            device_id_type=MESH,
        )

    if chips == 4:
        xn = s + 2 - 4 * ((s // 2) % 2)
        yn = (s + 4) % n
        dg = (xn + 4) % n

        def half(ref, item, i):
            rows = items[item][2] // 2
            return ref.at[pl.ds(i * rows, rows), :]

        def piece(item, sem, block, i, target, own=False):
            source, slot, _ = items[item]
            dest = half(slot(block), item, i)
            return copy(item, sem, half(source, item, i) if own else dest, dest, target)

        def across(item, sem, block, own=False):
            source, slot, _ = items[item]
            return copy(item, sem, source if own else slot(block), slot(block), twin)

        def other(block):
            return block + 1 - 2 * (block % CORES)

        def start(*these):
            for item in these:
                piece(item, 0, s, 0, xn, True).start()
                piece(item, 3, s, 1, yn, True).start()
            for item in these:
                piece(item, 1, s, 1, xn, True).start()
                piece(item, 2, s, 0, yn, True).start()
            for item in these:
                across(item, 6, s, True).start()

        def relay(item, stage):
            if stage == 0:
                piece(item, 0, xn, 0, xn).wait_recv()
                piece(item, 4, xn, 0, yn).start()
                piece(item, 3, yn, 1, yn).wait_recv()
                piece(item, 5, yn, 1, xn).start()
            elif stage == 1:
                piece(item, 1, xn, 1, xn).wait_recv()
                across(item, 7, xn).start()
                piece(item, 2, yn, 0, yn).wait_recv()
                across(item, 8, yn).start()
            else:
                piece(item, 4, dg, 0, yn).wait_recv()
                piece(item, 5, dg, 1, xn).wait_recv()
                across(item, 9, dg).start()

        def finish(item, near=True, far=True):
            for sem, block in ((6, s), (7, xn), (8, yn)) if near else ():
                across(item, sem, other(block)).wait_recv()
            if far:
                across(item, 9, other(dg)).wait_recv()

        def drain(item):
            piece(item, 0, s, 0, xn, True).wait_send()
            piece(item, 3, s, 1, yn, True).wait_send()
            piece(item, 1, s, 1, xn, True).wait_send()
            piece(item, 2, s, 0, yn, True).wait_send()
            piece(item, 4, xn, 0, yn).wait_send()
            piece(item, 5, yn, 1, xn).wait_send()
            across(item, 6, s, True).wait_send()
            for sem, block in ((7, xn), (8, yn), (9, dg)):
                across(item, sem, block).wait_send()

    else:

        def hop(item, kind, j, block, own, target):
            source, slot, _ = items[item]
            return copy(item, kind * chips + j, source if own else slot(block), slot(block), target)

        def start(*these):
            for item in these:
                for j in range(1, chips):
                    hop(item, 0, j, s, True, (s + CORES * j) % n).start()
                hop(item, 1, 0, s, True, twin).start()

        def relay(item, stage):
            if stage == 2:
                for j in range(1, chips):
                    origin = (s + n - CORES * j) % n
                    hop(item, 0, j, origin, False, origin).wait_recv()
                    hop(item, 1, j, origin, False, twin).start()

        def finish(item, near=True, far=True):
            for j in range(chips) if far else ():
                hop(item, 1, j, (twin + n - CORES * j) % n, False, twin).wait_recv()

        def drain(item):
            for j in range(1, chips):
                hop(item, 0, j, s, True, (s + CORES * j) % n).wait_send()
            hop(item, 1, 0, s, True, twin).wait_send()
            for j in range(1, chips):
                hop(item, 1, j, (s + n - CORES * j) % n, False, twin).wait_send()

    return start, relay, finish, drain


def line_sends(m, t, step):
    right = (t >= step) & (t < m - 1)
    left = (t + step < m) & (t > 0)
    return (right, 0, t - step, t + 1), (left, 1, t + step, t - 1)


def line_takes(m, t, step):
    return (
        (t - 1 - step >= 0, 0, t - 1 - step, t - 1),
        (t + 1 + step < m, 1, t + 1 + step, t + 1),
    )


def line_neighbours(m, t, act):
    @pl.when(t > 0)
    def _():
        act(t - 1)

    @pl.when(t < m - 1)
    def _():
        act(t + 1)


def project_kernel(
    n, m, tokens, w_query, w_key, w_value, w_out, gain, b_query, b_key, b_value, position, inv_freq,
    q, kv, w_mix, cosine, sine, tok_all, wq_all, wkv_all, acc, squares, scaled,
    plane_send, plane_recv, line_send, line_recv, mix_send, mix_recv, local_sem,
):
    s = lax.axis_index("seq")
    t = lax.axis_index("tensor")
    heads, rows, _ = q.shape
    kv_heads = kv.shape[0]
    depth, query_cols = w_query.shape
    key_cols = w_key.shape[1]
    feats = tokens.shape[1]
    g = n // m
    part = s % g
    home = s // g
    piece_rows = w_out.shape[0] // m

    barrier = pltpu.get_barrier_semaphore()
    partners = plane_partners(n, s)
    for other in partners:
        pl.semaphore_signal(barrier, inc=1, device_id={"seq": other}, device_id_type=MESH)
    line_neighbours(
        m, t, lambda o: pl.semaphore_signal(barrier, inc=1, device_id={"tensor": o}, device_id_type=MESH)
    )
    for p in range(m):

        @pl.when(home != p)
        def _():
            pl.semaphore_signal(barrier, inc=1, device_id={"seq": g * p + part}, device_id_type=MESH)

    ends = jnp.where(t > 0, 1, 0) + jnp.where(t < m - 1, 1, 0)
    pl.semaphore_wait(barrier, len(partners) + ends + (m - 1))

    def wq_slot(b):
        return wq_all.at[pl.ds(pl.multiple_of(b * depth, 128), depth), :]

    def wk_slot(b):
        return wkv_all.at[pl.ds(pl.multiple_of(b * depth, 128), depth), pl.ds(0, key_cols)]

    def wv_slot(b):
        return wkv_all.at[pl.ds(pl.multiple_of(b * depth, 128), depth), pl.ds(key_cols, key_cols)]

    items = [(w_query, wq_slot, depth), (w_key, wk_slot, depth), (w_value, wv_slot, depth)]
    start, relay, finish, drain = plane_gather(n, s, items, plane_send, plane_recv)

    parts = feats // depth
    chips = n // CORES

    def late(block):
        return block == chips - 1 - s // CORES if chips == 4 else block >= 0

    def line(way, step, part_of, block, first, target):
        return pltpu.make_async_remote_copy(
            src_ref=tokens.at[:, pl.ds(part_of * depth, depth)] if first else tok_all.at[block, part_of],
            dst_ref=tok_all.at[block, part_of],
            send_sem=line_send.at[way, step, part_of],
            recv_sem=line_recv.at[way, step, part_of],
            device_id={"tensor": target},
            device_id_type=MESH,
        )

    def send_line(step, part_of):
        for cond, way, block, target in line_sends(m, t, step):

            @pl.when(cond)
            def _():
                line(way, step, part_of, block, step == 0, target).start()

    def take_line(step, part_of):
        for valid, way, block, source in line_takes(m, t, step):

            @pl.when(valid)
            def _():
                line(way, step, part_of, block, False, source).wait_recv()

    for i in range(parts):
        send_line(0, i)
    start(0, 1, 2)

    def mix(p):
        return pltpu.make_async_remote_copy(
            src_ref=w_out.at[pl.ds(p * piece_rows, piece_rows), :],
            dst_ref=w_mix.at[home],
            send_sem=mix_send.at[p],
            recv_sem=mix_recv.at[home],
            device_id={"seq": g * p + part},
            device_id_type=MESH,
        )

    def mixed_in(f):
        return pltpu.make_async_remote_copy(
            src_ref=w_mix.at[f],
            dst_ref=w_mix.at[f],
            send_sem=mix_send.at[f],
            recv_sem=mix_recv.at[f],
            device_id={"seq": g * f + part},
            device_id_type=MESH,
        )

    own = [
        pltpu.make_async_copy(w_query, wq_slot(s), local_sem.at[0]),
        pltpu.make_async_copy(w_key, wk_slot(s), local_sem.at[1]),
        pltpu.make_async_copy(w_value, wv_slot(s), local_sem.at[2]),
    ]
    for i in range(parts):
        own.append(
            pltpu.make_async_copy(
                tokens.at[:, pl.ds(i * depth, depth)], tok_all.at[t, i], local_sem.at[3 + i]
            )
        )
    for copy in own:
        copy.start()
    acc[...] = jnp.zeros_like(acc)
    squares[...] = jnp.zeros_like(squares)

    def multiply(block, i):
        x = tok_all[block, i].astype(jnp.float32)
        sq = x * x
        total = sq[:, 0:128]
        for c in range(1, depth // 128):
            total = total + sq[:, c * 128 : (c + 1) * 128]
        squares[...] += total
        scaled[...] = (x * gain[block, i]).astype(jnp.bfloat16)
        row = pl.multiple_of(block * feats + i * depth, 128)
        half = query_cols // 2
        for c in range(2):
            cols = slice(c * half, (c + 1) * half)
            acc[:, cols] += jnp.dot(
                scaled[...], wq_all[pl.ds(row, depth), cols], preferred_element_type=jnp.float32
            )
        acc[:, query_cols:] += jnp.dot(
            scaled[...], wkv_all[pl.ds(row, depth), :], preferred_element_type=jnp.float32
        )

    def multiply_each(count, block_of, wanted):
        def one(i, _):
            block = block_of(i // parts)

            @pl.when((block >= 0) & (block < m) & wanted(block))
            def _():
                multiply(block, i % parts)

            return 0

        lax.fori_loop(0, count * parts, one, 0)

    place = position[...].astype(jnp.float32)
    angles = jnp.transpose(jnp.broadcast_to(place, (HD, rows))) * inv_freq[...]
    lane = lax.broadcasted_iota(jnp.int32, (rows, HD), 1)
    cosine[...] = jnp.cos(angles)
    turn = jnp.sin(angles)
    sine[...] = jnp.where(lane < HD // 2, -turn, turn)

    relay(0, 0)
    for i in range(parts):
        take_line(0, i)
        if m > 2:
            send_line(1, i)
        if i == 0:
            relay(1, 0)
            relay(2, 0)
    for item in range(3):
        relay(item, 1)
    for step in range(1, m - 2):
        for i in range(parts):
            take_line(step, i)
            send_line(step + 1, i)
    for p in range(m):

        @pl.when(home != p)
        def _():
            mix(p).start()

    for copy in own:
        copy.wait()
    for item in range(3):
        finish(item, far=False)

    def inside(block):
        return (block - t < m - 1) & (t - block < m - 1)

    multiply_each(m, lambda i: i, lambda b: jnp.logical_not(late(b)) & inside(b))
    for item in range(3):
        relay(item, 2)
    for item in range(3):
        finish(item, near=False)
    multiply_each(m, lambda i: i, lambda b: late(b) & inside(b))
    for i in range(parts):
        take_line(m - 2, i)

        def end(way, _):
            block = t + (2 * way - 1) * (m - 1)

            @pl.when((block >= 0) & (block < m))
            def _():
                multiply(block, i)

            return 0

        lax.fori_loop(0, 2, end, 0)

    mean = jnp.sum(squares[...], -1, keepdims=True) / (m * feats)
    inverse_rms = lax.rsqrt(mean + NORM_EPS)

    def head(i, bias, of):
        return acc[:, i * HD : (i + 1) * HD] * inverse_rms + bias[:, of * HD : (of + 1) * HD]

    def turned(i, bias, of):
        value = head(i, bias, of)
        return (value * cosine[...] + pltpu.roll(value, HD // 2, 1) * sine[...]).astype(jnp.bfloat16)

    for h in range(heads):
        q[h] = turned(h, b_query, h)
    for h in range(kv_heads):
        kv[h, :, 0:HD] = turned(heads + h, b_key, h)
        kv[h, :, HD : 2 * HD] = head(heads + kv_heads + h, b_value, h).astype(jnp.bfloat16)

    for item in range(3):
        drain(item)
    for p in range(m):

        @pl.when(home != p)
        def _():
            mix(p).wait_send()
            mixed_in(p).wait_recv()

    for step in range(m - 1):
        for cond, way, block, target in line_sends(m, t, step):

            @pl.when(cond)
            def _():
                for i in range(parts):
                    line(way, step, i, block, step == 0, target).wait_send()


def project(n, m, tokens, w_query, w_key, w_value, w_out, *small):
    rows, feats = tokens.shape
    depth, query_cols = w_query.shape
    key_cols = w_key.shape[1]
    heads, kv_heads = query_cols // HD, key_cols // HD
    parts = feats // depth
    wrows, wcols = w_out.shape
    bf16, f32 = jnp.bfloat16, jnp.float32
    dma = pltpu.SemaphoreType.DMA
    return pl.pallas_call(
        functools.partial(project_kernel, n, m),
        out_shape=(
            jax.ShapeDtypeStruct((heads, rows, HD), bf16),
            jax.ShapeDtypeStruct((kv_heads, rows, 2 * HD), bf16),
            jax.ShapeDtypeStruct((m, wrows // m, wcols), bf16),
        ),
        in_specs=[ANY] * 5 + [VMEM] * 6,
        out_specs=(VMEM, VMEM, ANY),
        scratch_shapes=[
            pltpu.VMEM((rows, HD), f32),
            pltpu.VMEM((rows, HD), f32),
            pltpu.VMEM((m, parts, rows, depth), bf16),
            pltpu.VMEM((n * depth, query_cols), bf16),
            pltpu.VMEM((n * depth, 2 * key_cols), bf16),
            pltpu.VMEM((rows, query_cols + 2 * key_cols), f32),
            pltpu.VMEM((rows, 128), f32),
            pltpu.VMEM((rows, depth), bf16),
            dma((3, plane_sems(n))),
            dma((3, plane_sems(n))),
            dma((2, m - 1, parts)),
            dma((2, m - 1, parts)),
            dma((m,)),
            dma((m,)),
            dma((3 + parts,)),
        ],
        compiler_params=pltpu.CompilerParams(
            collective_id=0, has_side_effects=True, vmem_limit_bytes=60 * 2**20
        ),
        cost_estimate=pl.CostEstimate(flops=10**11, bytes_accessed=10**8, transcendentals=0),
    )(tokens, w_query, w_key, w_value, w_out, *small)


def attend_kernel(
    n, m, q, kv, pos, tokens, w_out, w_mix, mixed, context,
    kv_all, pos_all, ctx_all, w_all, scores, biggest, total, acc, residual,
    plane_send, plane_recv, swap_send, swap_recv, line_send, line_recv, local_sem,
):
    s = lax.axis_index("seq")
    t = lax.axis_index("tensor")
    heads, rows, _ = q.shape
    kv_heads = kv.shape[0]
    group = heads // kv_heads
    g = n // m
    part = s % g
    home = s // g
    wrows, wcols = w_out.shape
    piece_rows = wrows // m
    chunks = heads // PAIR
    width = PAIR * HD
    outs = acc.shape[1]

    barrier = pltpu.get_barrier_semaphore()
    partners = plane_partners(n, s)
    for other in partners:
        pl.semaphore_signal(barrier, inc=1, device_id={"seq": other}, device_id_type=MESH)
    for other in range(m):

        @pl.when(t != other)
        def _():
            pl.semaphore_signal(barrier, inc=1, device_id={"tensor": other}, device_id_type=MESH)

    pl.semaphore_wait(barrier, len(partners) + m - 1)

    def kv_slot(h):
        return lambda b: kv_all.at[h, pl.ds(pl.multiple_of(b * rows, 128), rows), :]

    def w_slot(b, tt):
        return w_all.at[
            pl.ds(pl.multiple_of(tt * wrows + (b // g) * piece_rows, 16), piece_rows),
            pl.ds(pl.multiple_of((b % g) * wcols, 128), wcols),
        ]

    items = [(kv.at[h], kv_slot(h), rows) for h in range(kv_heads)]
    items.append((pos, lambda b: pos_all.at[b], pos.shape[0]))
    first_w = len(items)
    turn = 1 - 2 * (t // (m // 2))
    order = [(t + m + d * turn) % m for d in range(m)]
    for tt in order:
        items.append((w_slot(s, tt), lambda b, tt=tt: w_slot(b, tt), piece_rows))
    start, relay, finish, drain = plane_gather(n, s, items, plane_send, plane_recv)

    start(first_w - 1)
    for h in range(kv_heads):
        start(h)

    def swap(f, own):
        source = w_out.at[pl.ds(pl.multiple_of(home * piece_rows, 16), piece_rows), :]
        return pltpu.make_async_remote_copy(
            src_ref=source if own else w_mix.at[f],
            dst_ref=w_slot(s, t),
            send_sem=swap_send.at[f],
            recv_sem=swap_recv.at[t],
            device_id={"tensor": f},
            device_id_type=MESH,
        )

    def keep(own):
        source = w_out.at[pl.ds(pl.multiple_of(home * piece_rows, 16), piece_rows), :]
        return pltpu.make_async_copy(source if own else w_mix.at[t], w_slot(s, t), local_sem.at[0])

    for f in order[1:]:

        @pl.when(home == f)
        def _():
            swap(f, True).start()

        @pl.when(home != f)
        def _():
            swap(f, False).start()

    @pl.when(home == t)
    def _():
        keep(True).start()

    @pl.when(home != t)
    def _():
        keep(False).start()

    for h in range(kv_heads):
        kv_all[h, pl.ds(pl.multiple_of(s * rows, 128), rows), :] = kv[h]
    pos_all[s] = pos[...]

    load = pltpu.make_async_copy(tokens, residual, local_sem.at[1])
    load.start()

    def arrived(tt):
        pltpu.make_async_remote_copy(
            src_ref=w_slot(s, tt),
            dst_ref=w_slot(s, tt),
            send_sem=swap_send.at[tt],
            recv_sem=swap_recv.at[tt],
            device_id={"tensor": tt},
            device_id_type=MESH,
        ).wait_recv()

    def line(way, step, chunk, block, target):
        return pltpu.make_async_remote_copy(
            src_ref=ctx_all.at[block, chunk],
            dst_ref=ctx_all.at[block, chunk],
            send_sem=line_send.at[way, step, chunk],
            recv_sem=line_recv.at[way, step, chunk],
            device_id={"tensor": target},
            device_id_type=MESH,
        )

    def send_line(step, chunk):
        for cond, way, block, target in line_sends(m, t, step):

            @pl.when(cond)
            def _():
                line(way, step, chunk, block, target).start()

    mine = jnp.broadcast_to(pos[0:1, :].astype(jnp.float32), (128, rows))
    query_pos = jnp.transpose(mine)[:, 0:1].astype(jnp.int32)
    scale = HD ** (-0.5) * 1.4426950408889634

    def attend(h):
        base = h // group

        def block_scores(b, _):
            at = pl.multiple_of(b * rows, 128)
            keys = kv_all[base, pl.ds(at, rows), 0:HD]
            raw = lax.dot_general(
                q[h], keys, (((1,), (1,)), ((), ())), preferred_element_type=jnp.float32
            )
            masked = jnp.where(pos_all[b, 0:1, :] <= query_pos, raw, NEG_FILL)
            scores[b] = masked
            top = biggest[...]
            for i in range(rows // 128):
                top = jnp.maximum(top, masked[:, i * 128 : (i + 1) * 128])
            biggest[...] = top
            return 0

        biggest[...] = jnp.full_like(biggest, NEG_FILL)
        lax.fori_loop(0, n, block_scores, 0)
        row_max = jnp.max(biggest[...], -1, keepdims=True) * scale
        total[...] = jnp.zeros_like(total)
        biggest[...] = jnp.zeros_like(biggest)

        def block_values(b, _):
            at = pl.multiple_of(b * rows, 128)
            weights = jnp.exp2(scores[b] * scale - row_max)
            value = kv_all[base, pl.ds(at, rows), HD : 2 * HD]
            total[...] += jnp.dot(
                weights.astype(jnp.bfloat16), value, preferred_element_type=jnp.float32
            )
            add = weights[:, 0:128]
            for i in range(1, rows // 128):
                add = add + weights[:, i * 128 : (i + 1) * 128]
            biggest[...] += add
            return 0

        lax.fori_loop(0, n, block_values, 0)
        denominator = jnp.sum(biggest[...], -1, keepdims=True)
        return (total[...] / denominator).astype(jnp.bfloat16)

    for stage in range(3):
        relay(first_w - 1, stage)
        relay(0, stage)
    for h in range(1, kv_heads):
        relay(h, 0)
    keep(True).wait()
    start(first_w)
    finish(first_w - 1)

    work = []
    for d in range(1, m):
        work.append([("start", d), ("relay", d - 1, 0)])
        if d > 1:
            work[-1].append(("relay", d - 2, 1))
        if d > 2:
            work[-1].append(("relay", d - 3, 2))

    def advance(jobs):
        for job in jobs:
            if job[0] == "start":
                arrived(order[job[1]])
                start(first_w + job[1])
            else:
                relay(first_w + job[1], job[2])

    rest = []
    for d in range(m):
        for stage in range(3):
            if all(("relay", d, stage) not in jobs for jobs in work):
                rest.append((d + stage, d, ("relay", d, stage)))
    rest = [job for _, _, job in sorted(rest)]

    def take_line(step, chunk):
        for valid, way, block, source in line_takes(m, t, step):

            @pl.when(valid)
            def _():
                line(way, step, chunk, block, source).wait_recv()

            if step + 1 < m - 1:
                go = valid & ((t < m - 1) if way == 0 else (t > 0))
                onward = t + 1 if way == 0 else t - 1

                @pl.when(go)
                def _():
                    line(way, step + 1, chunk, block, onward).start()

    takes = [[] for _ in range(chunks + m)]
    for step in range(m - 2):
        for chunk in range(chunks):
            takes[chunk + step + 1].append((step, chunk))

    stored = []
    for chunk in range(chunks):
        base = chunk * PAIR // group
        if chunk * PAIR % group == 0:
            finish(base)

        def one(i, _):
            value = attend(chunk * PAIR + i)
            ctx_all[t, chunk, :, pl.ds(pl.multiple_of(i * HD, HD), HD)] = value
            return 0

        lax.fori_loop(0, PAIR, one, 0)
        send_line(0, chunk)
        out = pltpu.make_async_copy(
            ctx_all.at[t, chunk],
            context.at[:, pl.ds(chunk * width, width)],
            local_sem.at[2 + chunk],
        )
        out.start()
        stored.append(out)
        for take in takes[chunk]:
            take_line(*take)
        if chunk * PAIR % group == 0 and base + 1 < kv_heads:
            relay(base + 1, 1)
            relay(base + 1, 2)
        if chunk < len(work):
            advance(work[chunk])
    for jobs in work[chunks:]:
        advance(jobs)

    load.wait()

    def out_proj(block, first):
        for j in range(outs // wcols):
            cols = slice(j * wcols, (j + 1) * wcols)

            def partial(c):
                at = pl.multiple_of(block * wrows + c * width, 128)
                return jnp.dot(
                    ctx_all[block, c], w_all[pl.ds(at, width), cols], preferred_element_type=jnp.float32
                )

            value = partial(0)
            for c in range(1, chunks):
                value = value + partial(c)
            acc[:, cols] = value + (residual[:, cols].astype(jnp.float32) if first else acc[:, cols])

    def add_blocks(step):
        def way(i, _):
            block = jnp.where(i == 0, t - 1 - step, t + 1 + step)

            @pl.when((block >= 0) & (block < m))
            def _():
                out_proj(block, False)

            return 0

        lax.fori_loop(0, 2, way, 0)

    ahead = takes[chunks:]
    per = (len(rest) + len(ahead) - 1) // len(ahead)
    for i, group_of in enumerate(ahead):
        for take in group_of:
            take_line(*take)
        advance(rest[i * per : (i + 1) * per])
    for d in range(m):
        finish(first_w + d)
    out_proj(t, True)
    for step in range(m - 1):
        if step == m - 2:
            for chunk in range(chunks):
                take_line(step, chunk)
        add_blocks(step)

    residual[...] = acc[...].astype(jnp.bfloat16)
    final = pltpu.make_async_copy(residual, mixed, local_sem.at[1])
    final.start()

    for item in range(len(items)):
        drain(item)
    for f in order[1:]:
        swap(f, False).wait_send()

    for step in range(m - 1):
        for cond, way, block, target in line_sends(m, t, step):
            for chunk in range(chunks):

                @pl.when(cond)
                def _():
                    line(way, step, chunk, block, target).wait_send()

    for out in stored:
        out.wait()
    final.wait()


def attend_and_mix(n, m, q, kv, pos, tokens, w_out, w_mix):
    heads, rows, _ = q.shape
    kv_heads = kv.shape[0]
    wrows, wcols = w_out.shape
    outs = tokens.shape[1]
    chunks = heads // PAIR
    items = kv_heads + 1 + m
    bf16, f32 = jnp.bfloat16, jnp.float32
    dma = pltpu.SemaphoreType.DMA
    return pl.pallas_call(
        functools.partial(attend_kernel, n, m),
        out_shape=(
            jax.ShapeDtypeStruct(tokens.shape, bf16),
            jax.ShapeDtypeStruct((rows, heads * HD), bf16),
        ),
        in_specs=[VMEM, VMEM, VMEM, ANY, ANY, ANY],
        out_specs=(ANY, ANY),
        scratch_shapes=[
            pltpu.VMEM((kv_heads, n * rows, 2 * HD), bf16),
            pltpu.VMEM((n, *pos.shape), pos.dtype),
            pltpu.VMEM((m, chunks, rows, PAIR * HD), bf16),
            pltpu.VMEM((m * wrows, outs), bf16),
            pltpu.VMEM((n, rows, rows), f32),
            pltpu.VMEM((rows, 128), f32),
            pltpu.VMEM((rows, HD), f32),
            pltpu.VMEM((rows, outs), f32),
            pltpu.VMEM((rows, outs), bf16),
            dma((items, plane_sems(n))),
            dma((items, plane_sems(n))),
            dma((m,)),
            dma((m,)),
            dma((2, m - 1, chunks)),
            dma((2, m - 1, chunks)),
            dma((2 + chunks,)),
        ],
        compiler_params=pltpu.CompilerParams(
            collective_id=1, has_side_effects=True, vmem_limit_bytes=60 * 2**20
        ),
        cost_estimate=pl.CostEstimate(flops=10**11, bytes_accessed=10**8, transcendentals=0),
    )(q, kv, pos, tokens, w_out, w_mix)


def shards(seq, tensor, tokens, positions, norm_gain, w_query, w_key, w_value, b_query, b_key, b_value, w_out):
    rows, feats = tokens.shape
    half = HD // 2
    inv_freq = ROPE_BASE ** (-jnp.arange(half, dtype=jnp.float32) * 2.0 / HD)
    inv_freq = jnp.concatenate((inv_freq, inv_freq))
    pos = jnp.broadcast_to(positions[None, :], (16, rows))
    q, kv, w_mix = project(
        seq, tensor, tokens, w_query, w_key, w_value, w_out,
        norm_gain.reshape(tensor, feats // w_query.shape[0], 1, w_query.shape[0]),
        b_query[None, :], b_key[None, :], b_value[None, :], positions[None, :], inv_freq[None, :],
    )
    return attend_and_mix(seq, tensor, q, kv, pos, tokens, w_out, w_mix)


def solution(mesh):
    in_specs = (
        P("seq", "tensor"),
        P("seq"),
        P(),
        P("seq", "tensor"),
        P("seq", "tensor"),
        P("seq", "tensor"),
        P("tensor"),
        P("tensor"),
        P("tensor"),
        P("tensor", "seq"),
    )
    out_specs = (P("seq", "tensor"), P("seq", "tensor"))

    def body(*args):
        return shards(mesh.shape["seq"], mesh.shape["tensor"], *args)

    return jax.shard_map(body, mesh=mesh, in_specs=in_specs, out_specs=out_specs, check_vma=False)
```

```python
import functools

import jax
import jax.numpy as jnp
from jax import lax
from jax.experimental import pallas as pl
from jax.experimental.pallas import tpu as pltpu
from jax.sharding import PartitionSpec as P

HD = 128


NORM_EPS = 1e-06
ROPE_BASE = 1000000.0
NEG_FILL = -1e30
CORES = 2
PLANE_SEMS = 10
MESH = pl.DeviceIdType.MESH
ANY = pl.BlockSpec(memory_space=pl.ANY)
VMEM = pl.BlockSpec(memory_space=pltpu.VMEM)


def plane_sems(n):
    chips = n // CORES
    return PLANE_SEMS if chips == 4 else 2 * chips


def plane_partners(n, s):
    twin = s + 1 - 2 * (s % CORES)
    chips = n // CORES
    if chips == 4:
        return [twin, s + 2 - 4 * ((s // 2) % 2), (s + 4) % n]
    return [twin] + [(s + CORES * j) % n for j in range(1, chips)]


def plane_gather(n, s, items, send_sem, recv_sem):
    twin = s + 1 - 2 * (s % CORES)
    chips = n // CORES

    def copy(item, sem, source, dest, target):
        return pltpu.make_async_remote_copy(
            src_ref=source,
            dst_ref=dest,
            send_sem=send_sem.at[item, sem],
            recv_sem=recv_sem.at[item, sem],
            device_id={"seq": target},
            device_id_type=MESH,
        )

    if chips == 4:
        xn = s + 2 - 4 * ((s // 2) % 2)
        yn = (s + 4) % n
        dg = (xn + 4) % n

        def half(ref, item, i):
            rows = items[item][2] // 2
            return ref.at[pl.ds(i * rows, rows), :]

        def piece(item, sem, block, i, target, own=False):
            source, slot, _ = items[item]
            dest = half(slot(block), item, i)
            return copy(item, sem, half(source, item, i) if own else dest, dest, target)

        def across(item, sem, block, own=False):
            source, slot, _ = items[item]
            return copy(item, sem, source if own else slot(block), slot(block), twin)

        def other(block):
            return block + 1 - 2 * (block % CORES)

        def start(*these):
            for item in these:
                piece(item, 0, s, 0, xn, True).start()
                piece(item, 3, s, 1, yn, True).start()
            for item in these:
                piece(item, 1, s, 1, xn, True).start()
                piece(item, 2, s, 0, yn, True).start()
            for item in these:
                across(item, 6, s, True).start()

        def relay(item, stage):
            if stage == 0:
                piece(item, 0, xn, 0, xn).wait_recv()
                piece(item, 4, xn, 0, yn).start()
                piece(item, 3, yn, 1, yn).wait_recv()
                piece(item, 5, yn, 1, xn).start()
            elif stage == 1:
                piece(item, 1, xn, 1, xn).wait_recv()
                across(item, 7, xn).start()
                piece(item, 2, yn, 0, yn).wait_recv()
                across(item, 8, yn).start()
            else:
                piece(item, 4, dg, 0, yn).wait_recv()
                piece(item, 5, dg, 1, xn).wait_recv()
                across(item, 9, dg).start()

        def finish(item, near=True, far=True):
            for sem, block in ((6, s), (7, xn), (8, yn)) if near else ():
                across(item, sem, other(block)).wait_recv()
            if far:
                across(item, 9, other(dg)).wait_recv()

        def drain(item):
            piece(item, 0, s, 0, xn, True).wait_send()
            piece(item, 3, s, 1, yn, True).wait_send()
            piece(item, 1, s, 1, xn, True).wait_send()
            piece(item, 2, s, 0, yn, True).wait_send()
            piece(item, 4, xn, 0, yn).wait_send()
            piece(item, 5, yn, 1, xn).wait_send()
            across(item, 6, s, True).wait_send()
            for sem, block in ((7, xn), (8, yn), (9, dg)):
                across(item, sem, block).wait_send()

    else:

        def hop(item, kind, j, block, own, target):
            source, slot, _ = items[item]
            return copy(item, kind * chips + j, source if own else slot(block), slot(block), target)

        def start(*these):
            for item in these:
                for j in range(1, chips):
                    hop(item, 0, j, s, True, (s + CORES * j) % n).start()
                hop(item, 1, 0, s, True, twin).start()

        def relay(item, stage):
            if stage == 2:
                for j in range(1, chips):
                    origin = (s + n - CORES * j) % n
                    hop(item, 0, j, origin, False, origin).wait_recv()
                    hop(item, 1, j, origin, False, twin).start()

        def finish(item, near=True, far=True):
            for j in range(chips) if far else ():
                hop(item, 1, j, (twin + n - CORES * j) % n, False, twin).wait_recv()

        def drain(item):
            for j in range(1, chips):
                hop(item, 0, j, s, True, (s + CORES * j) % n).wait_send()
            hop(item, 1, 0, s, True, twin).wait_send()
            for j in range(1, chips):
                hop(item, 1, j, (s + n - CORES * j) % n, False, twin).wait_send()

    return start, relay, finish, drain


def line_sends(m, t, step):
    right = (t >= step) & (t < m - 1)
    left = (t + step < m) & (t > 0)
    return (right, 0, t - step, t + 1), (left, 1, t + step, t - 1)


def line_takes(m, t, step):
    return (
        (t - 1 - step >= 0, 0, t - 1 - step, t - 1),
        (t + 1 + step < m, 1, t + 1 + step, t + 1),
    )


def line_neighbours(m, t, act):
    @pl.when(t > 0)
    def _():
        act(t - 1)

    @pl.when(t < m - 1)
    def _():
        act(t + 1)


def project_kernel(
    n, m, tokens, w_query, w_key, w_value, w_out, gain, b_query, b_key, b_value, position, inv_freq,
    q, kv, w_mix, w_near, cosine, sine, tok_all, wq_all, wkv_all, acc, squares, scaled,
    plane_send, plane_recv, line_send, line_recv, mix_send, mix_recv, near_send, near_recv, local_sem,
):
    s = lax.axis_index("seq")
    t = lax.axis_index("tensor")
    heads, rows, _ = q.shape
    kv_heads = kv.shape[0]
    depth, query_cols = w_query.shape
    key_cols = w_key.shape[1]
    feats = tokens.shape[1]
    g = n // m
    part = s % g
    home = s // g
    piece_rows = w_out.shape[0] // m

    barrier = pltpu.get_barrier_semaphore()
    partners = plane_partners(n, s)
    for other in partners:
        pl.semaphore_signal(barrier, inc=1, device_id={"seq": other}, device_id_type=MESH)
    line_neighbours(
        m, t, lambda o: pl.semaphore_signal(barrier, inc=1, device_id={"tensor": o}, device_id_type=MESH)
    )
    for p in range(m):

        @pl.when(home != p)
        def _():
            pl.semaphore_signal(barrier, inc=1, device_id={"seq": g * p + part}, device_id_type=MESH)

    ends = jnp.where(t > 0, 1, 0) + jnp.where(t < m - 1, 1, 0)
    pl.semaphore_wait(barrier, len(partners) + ends + (m - 1))

    def wq_slot(b):
        return wq_all.at[pl.ds(pl.multiple_of(b * depth, 128), depth), :]

    def wk_slot(b):
        return wkv_all.at[pl.ds(pl.multiple_of(b * depth, 128), depth), pl.ds(0, key_cols)]

    def wv_slot(b):
        return wkv_all.at[pl.ds(pl.multiple_of(b * depth, 128), depth), pl.ds(key_cols, key_cols)]

    items = [(w_query, wq_slot, depth), (w_key, wk_slot, depth), (w_value, wv_slot, depth)]
    start, relay, finish, drain = plane_gather(n, s, items, plane_send, plane_recv)

    parts = feats // depth
    chips = n // CORES

    def late(block):
        return block == chips - 1 - s // CORES if chips == 4 else block >= 0

    def line(way, step, part_of, block, first, target):
        return pltpu.make_async_remote_copy(
            src_ref=tokens.at[:, pl.ds(part_of * depth, depth)] if first else tok_all.at[block, part_of],
            dst_ref=tok_all.at[block, part_of],
            send_sem=line_send.at[way, step, part_of],
            recv_sem=line_recv.at[way, step, part_of],
            device_id={"tensor": target},
            device_id_type=MESH,
        )

    def send_line(step, part_of):
        for cond, way, block, target in line_sends(m, t, step):

            @pl.when(cond)
            def _():
                line(way, step, part_of, block, step == 0, target).start()

    def take_line(step, part_of):
        for valid, way, block, source in line_takes(m, t, step):

            @pl.when(valid)
            def _():
                line(way, step, part_of, block, False, source).wait_recv()

    for i in range(parts):
        send_line(0, i)
    start(0, 1, 2)

    def mix(p):
        return pltpu.make_async_remote_copy(
            src_ref=w_out.at[pl.ds(p * piece_rows, piece_rows), :],
            dst_ref=w_mix.at[home],
            send_sem=mix_send.at[p],
            recv_sem=mix_recv.at[home],
            device_id={"seq": g * p + part},
            device_id_type=MESH,
        )

    def mixed_in(f):
        return pltpu.make_async_remote_copy(
            src_ref=w_mix.at[f],
            dst_ref=w_mix.at[f],
            send_sem=mix_send.at[f],
            recv_sem=mix_recv.at[f],
            device_id={"seq": g * f + part},
            device_id_type=MESH,
        )

    own = [
        pltpu.make_async_copy(w_query, wq_slot(s), local_sem.at[0]),
        pltpu.make_async_copy(w_key, wk_slot(s), local_sem.at[1]),
        pltpu.make_async_copy(w_value, wv_slot(s), local_sem.at[2]),
    ]
    for i in range(parts):
        own.append(
            pltpu.make_async_copy(
                tokens.at[:, pl.ds(i * depth, depth)], tok_all.at[t, i], local_sem.at[3 + i]
            )
        )
    for copy in own:
        copy.start()
    acc[...] = jnp.zeros_like(acc)
    squares[...] = jnp.zeros_like(squares)

    def multiply(block, i):
        x = tok_all[block, i].astype(jnp.float32)
        sq = x * x
        total = sq[:, 0:128]
        for c in range(1, depth // 128):
            total = total + sq[:, c * 128 : (c + 1) * 128]
        squares[...] += total
        scaled[...] = (x * gain[block, i]).astype(jnp.bfloat16)
        row = pl.multiple_of(block * feats + i * depth, 128)
        half = query_cols // 2
        for c in range(2):
            cols = slice(c * half, (c + 1) * half)
            acc[:, cols] += jnp.dot(
                scaled[...], wq_all[pl.ds(row, depth), cols], preferred_element_type=jnp.float32
            )
        acc[:, query_cols:] += jnp.dot(
            scaled[...], wkv_all[pl.ds(row, depth), :], preferred_element_type=jnp.float32
        )

    def multiply_each(count, block_of, wanted):
        def one(i, _):
            block = block_of(i // parts)

            @pl.when((block >= 0) & (block < m) & wanted(block))
            def _():
                multiply(block, i % parts)

            return 0

        lax.fori_loop(0, count * parts, one, 0)

    place = position[...].astype(jnp.float32)
    angles = jnp.transpose(jnp.broadcast_to(place, (HD, rows))) * inv_freq[...]
    lane = lax.broadcasted_iota(jnp.int32, (rows, HD), 1)
    cosine[...] = jnp.cos(angles)
    turn = jnp.sin(angles)
    sine[...] = jnp.where(lane < HD // 2, -turn, turn)

    relay(0, 0)
    for i in range(parts):
        take_line(0, i)
        if m > 2:
            send_line(1, i)
        if i == 0:
            relay(1, 0)
            relay(2, 0)
    for item in range(3):
        relay(item, 1)
    for step in range(1, m - 2):
        for i in range(parts):
            take_line(step, i)
            send_line(step + 1, i)
    for p in range(m):

        @pl.when(home != p)
        def _():
            mix(p).start()

    for copy in own:
        copy.wait()
    for item in range(3):
        finish(item, far=False)

    def inside(block):
        return (block - t < m - 1) & (t - block < m - 1)

    multiply_each(m, lambda i: i, lambda b: jnp.logical_not(late(b)) & inside(b))
    for item in range(3):
        relay(item, 2)
    for item in range(3):
        finish(item, near=False)
    multiply_each(m, lambda i: i, lambda b: late(b) & inside(b))
    for p in range(m):

        @pl.when(home != p)
        def _():
            mixed_in(p).wait_recv()

    inner = (t > 0) & (t < m - 1)
    def near(way, own):
        to = t + 1 - 2 * way
        source = w_out.at[pl.ds(pl.multiple_of(home * piece_rows, 16), piece_rows), :]
        return pltpu.make_async_remote_copy(
            src_ref=source if own else w_mix.at[to],
            dst_ref=w_near.at[way],
            send_sem=near_send.at[way],
            recv_sem=near_recv.at[way],
            device_id={"tensor": to},
            device_id_type=MESH,
        )

    sides = ((0, t < m - 2, inner), (1, t > 1, inner))
    for way, gives, _ in sides:

        @pl.when(gives & (home == t + 1 - 2 * way))
        def _():
            near(way, True).start()

        @pl.when(gives & (home != t + 1 - 2 * way))
        def _():
            near(way, False).start()

    for i in range(parts):
        take_line(m - 2, i)

        def end(way, _):
            block = t + (2 * way - 1) * (m - 1)

            @pl.when((block >= 0) & (block < m))
            def _():
                multiply(block, i)

            return 0

        lax.fori_loop(0, 2, end, 0)

    mean = jnp.sum(squares[...], -1, keepdims=True) / (m * feats)
    inverse_rms = lax.rsqrt(mean + NORM_EPS)

    def head(i, bias, of):
        return acc[:, i * HD : (i + 1) * HD] * inverse_rms + bias[:, of * HD : (of + 1) * HD]

    def turned(i, bias, of):
        value = head(i, bias, of)
        return (value * cosine[...] + pltpu.roll(value, HD // 2, 1) * sine[...]).astype(jnp.bfloat16)

    for h in range(heads):
        q[h] = turned(h, b_query, h)
    for h in range(kv_heads):
        kv[h, :, 0:HD] = turned(heads + h, b_key, h)
        kv[h, :, HD : 2 * HD] = head(heads + kv_heads + h, b_value, h).astype(jnp.bfloat16)

    for item in range(3):
        drain(item)
    for p in range(m):

        @pl.when(home != p)
        def _():
            mix(p).wait_send()

    for way, gives, gets in sides:

        @pl.when(gives)
        def _():
            near(way, True).wait_send()

        @pl.when(gets)
        def _():
            pltpu.make_async_remote_copy(
                src_ref=w_near.at[way],
                dst_ref=w_near.at[way],
                send_sem=near_send.at[way],
                recv_sem=near_recv.at[way],
                device_id={"tensor": t - 1 + 2 * way},
                device_id_type=MESH,
            ).wait_recv()

    for step in range(m - 1):
        for cond, way, block, target in line_sends(m, t, step):

            @pl.when(cond)
            def _():
                for i in range(parts):
                    line(way, step, i, block, step == 0, target).wait_send()


def project(n, m, tokens, w_query, w_key, w_value, w_out, *small):
    rows, feats = tokens.shape
    depth, query_cols = w_query.shape
    key_cols = w_key.shape[1]
    heads, kv_heads = query_cols // HD, key_cols // HD
    parts = feats // depth
    wrows, wcols = w_out.shape
    bf16, f32 = jnp.bfloat16, jnp.float32
    dma = pltpu.SemaphoreType.DMA
    return pl.pallas_call(
        functools.partial(project_kernel, n, m),
        out_shape=(
            jax.ShapeDtypeStruct((heads, rows, HD), bf16),
            jax.ShapeDtypeStruct((kv_heads, rows, 2 * HD), bf16),
            jax.ShapeDtypeStruct((m, wrows // m, wcols), bf16),
            jax.ShapeDtypeStruct((2, wrows // m, wcols), bf16),
        ),
        in_specs=[ANY] * 5 + [VMEM] * 6,
        out_specs=(VMEM, VMEM, ANY, ANY),
        scratch_shapes=[
            pltpu.VMEM((rows, HD), f32),
            pltpu.VMEM((rows, HD), f32),
            pltpu.VMEM((m, parts, rows, depth), bf16),
            pltpu.VMEM((n * depth, query_cols), bf16),
            pltpu.VMEM((n * depth, 2 * key_cols), bf16),
            pltpu.VMEM((rows, query_cols + 2 * key_cols), f32),
            pltpu.VMEM((rows, 128), f32),
            pltpu.VMEM((rows, depth), bf16),
            dma((3, plane_sems(n))),
            dma((3, plane_sems(n))),
            dma((2, m - 1, parts)),
            dma((2, m - 1, parts)),
            dma((m,)),
            dma((m,)),
            dma((2,)),
            dma((2,)),
            dma((3 + parts,)),
        ],
        compiler_params=pltpu.CompilerParams(
            collective_id=0, has_side_effects=True, vmem_limit_bytes=60 * 2**20
        ),
        cost_estimate=pl.CostEstimate(flops=10**11, bytes_accessed=10**8, transcendentals=0),
    )(tokens, w_query, w_key, w_value, w_out, *small)


def attend_kernel(
    n, m, q, kv, pos, tokens, w_out, w_mix, w_near, mixed, context,
    kv_all, pos_all, ctx_all, w_all, scores, biggest, total, acc, residual,
    plane_send, plane_recv, swap_send, swap_recv, line_send, line_recv, near_sem, local_sem,
):
    s = lax.axis_index("seq")
    t = lax.axis_index("tensor")
    heads, rows, _ = q.shape
    kv_heads = kv.shape[0]
    group = heads // kv_heads
    g = n // m
    part = s % g
    home = s // g
    wrows, wcols = w_out.shape
    piece_rows = wrows // m
    outs = acc.shape[1]

    barrier = pltpu.get_barrier_semaphore()
    partners = plane_partners(n, s)
    for other in partners:
        pl.semaphore_signal(barrier, inc=1, device_id={"seq": other}, device_id_type=MESH)
    for other in range(m):

        @pl.when(t != other)
        def _():
            pl.semaphore_signal(barrier, inc=1, device_id={"tensor": other}, device_id_type=MESH)

    pl.semaphore_wait(barrier, len(partners) + m - 1)

    def kv_slot(h):
        return lambda b: kv_all.at[h, pl.ds(pl.multiple_of(b * rows, 128), rows), :]

    def w_slot(b, tt):
        return w_all.at[
            pl.ds(pl.multiple_of(tt * wrows + (b // g) * piece_rows, 16), piece_rows),
            pl.ds(pl.multiple_of((b % g) * wcols, 128), wcols),
        ]

    items = [(kv.at[h], kv_slot(h), rows) for h in range(kv_heads)]
    items.append((pos, lambda b: pos_all.at[b], pos.shape[0]))
    first_w = len(items)
    turn = 1 - 2 * (t // (m // 2))
    order = [(t + m + d * turn) % m for d in range(m)]
    for tt in order:
        items.append((w_slot(s, tt), lambda b, tt=tt: w_slot(b, tt), piece_rows))
    start, relay, finish, drain = plane_gather(n, s, items, plane_send, plane_recv)

    start(first_w - 1)
    for h in range(kv_heads):
        start(h)

    def swap(f, own):
        source = w_out.at[pl.ds(pl.multiple_of(home * piece_rows, 16), piece_rows), :]
        return pltpu.make_async_remote_copy(
            src_ref=source if own else w_mix.at[f],
            dst_ref=w_slot(s, t),
            send_sem=swap_send.at[f],
            recv_sem=swap_recv.at[t],
            device_id={"tensor": f},
            device_id_type=MESH,
        )

    def keep(own):
        source = w_out.at[pl.ds(pl.multiple_of(home * piece_rows, 16), piece_rows), :]
        return pltpu.make_async_copy(source if own else w_mix.at[t], w_slot(s, t), local_sem.at[0])

    def beside(way):
        return pltpu.make_async_copy(w_near.at[way], w_slot(s, t - 1 + 2 * way), near_sem.at[way])

    inner = (t > 0) & (t < m - 1)

    def apart(f):
        return (f - t > 1) | (t - f > 1)

    def far(f):
        return apart(f) | (f == 0) | (f == m - 1)

    for f in order[1:]:

        @pl.when(far(f) & (home == f))
        def _():
            swap(f, True).start()

        @pl.when(far(f) & (home != f))
        def _():
            swap(f, False).start()

    @pl.when(inner)
    def _():
        beside(0).start()
        beside(1).start()

    @pl.when(home == t)
    def _():
        keep(True).start()

    @pl.when(home != t)
    def _():
        keep(False).start()

    for h in range(kv_heads):
        kv_all[h, pl.ds(pl.multiple_of(s * rows, 128), rows), :] = kv[h]
    pos_all[s] = pos[...]

    load = pltpu.make_async_copy(tokens, residual, local_sem.at[1])
    load.start()

    def arrived(tt):
        @pl.when(inner & (tt == t - 1))
        def _():
            beside(0).wait()

        @pl.when(inner & (tt == t + 1))
        def _():
            beside(1).wait()

        @pl.when(apart(tt) | jnp.logical_not(inner))
        def _():
            pltpu.make_async_remote_copy(
                src_ref=w_slot(s, tt),
                dst_ref=w_slot(s, tt),
                send_sem=swap_send.at[tt],
                recv_sem=swap_recv.at[tt],
                device_id={"tensor": tt},
                device_id_type=MESH,
            ).wait_recv()

    def line(way, step, chunk, block, target):
        return pltpu.make_async_remote_copy(
            src_ref=ctx_all.at[block, :, pl.ds(chunk * HD, HD)],
            dst_ref=ctx_all.at[block, :, pl.ds(chunk * HD, HD)],
            send_sem=line_send.at[way, step, chunk],
            recv_sem=line_recv.at[way, step, chunk],
            device_id={"tensor": target},
            device_id_type=MESH,
        )

    def send_line(step, chunk):
        for cond, way, block, target in line_sends(m, t, step):

            @pl.when(cond)
            def _():
                line(way, step, chunk, block, target).start()

    mine = jnp.broadcast_to(pos[0:1, :].astype(jnp.float32), (128, rows))
    query_pos = jnp.transpose(mine)[:, 0:1].astype(jnp.int32)
    scale = HD ** (-0.5) * 1.4426950408889634

    def attend(h):
        base = h // group

        def block_scores(b, _):
            at = pl.multiple_of(b * rows, 128)
            keys = kv_all[base, pl.ds(at, rows), 0:HD]
            raw = lax.dot_general(
                q[h], keys, (((1,), (1,)), ((), ())), preferred_element_type=jnp.float32
            )
            masked = jnp.where(pos_all[b, 0:1, :] <= query_pos, raw, NEG_FILL)
            scores[b] = masked
            top = biggest[...]
            for i in range(rows // 128):
                top = jnp.maximum(top, masked[:, i * 128 : (i + 1) * 128])
            biggest[...] = top
            return 0

        biggest[...] = jnp.full_like(biggest, NEG_FILL)
        lax.fori_loop(0, n, block_scores, 0)
        row_max = jnp.max(biggest[...], -1, keepdims=True) * scale
        total[...] = jnp.zeros_like(total)
        biggest[...] = jnp.zeros_like(biggest)

        def block_values(b, _):
            at = pl.multiple_of(b * rows, 128)
            weights = jnp.exp2(scores[b] * scale - row_max)
            value = kv_all[base, pl.ds(at, rows), HD : 2 * HD]
            total[...] += jnp.dot(
                weights.astype(jnp.bfloat16), value, preferred_element_type=jnp.float32
            )
            add = weights[:, 0:128]
            for i in range(1, rows // 128):
                add = add + weights[:, i * 128 : (i + 1) * 128]
            biggest[...] += add
            return 0

        lax.fori_loop(0, n, block_values, 0)
        denominator = jnp.sum(biggest[...], -1, keepdims=True)
        return (total[...] / denominator).astype(jnp.bfloat16)

    for stage in range(3):
        relay(first_w - 1, stage)
        relay(0, stage)
    for h in range(1, kv_heads):
        relay(h, 0)
    keep(True).wait()
    start(first_w)
    finish(first_w - 1)

    ready = {d: 2 * d - 2 for d in range(1, m)}
    due = [[] for _ in range(heads + 2 * m + 4)]
    for chunk in range(heads):
        for step in range(m - 2):
            due[chunk + 1 + step].append((0, step, chunk))
    for d in range(m):
        if d:
            due[ready[d]].append((1, d))
        for stage in range(3):
            due[ready.get(d, -1) + 1 + stage].append((2, d, stage))
    for h in range(1, kv_heads):
        for stage in (1, 2):
            due[(h - 1) * group + stage - 1].append((3, h, stage))

    def advance(jobs):
        for job in sorted(jobs):
            if job[0] == 0:
                take_line(*job[1:])
            elif job[0] == 1:
                arrived(order[job[1]])
                start(first_w + job[1])
            elif job[0] == 2:
                relay(first_w + job[1], job[2])
            else:
                relay(job[1], job[2])

    def take_line(step, chunk):
        for valid, way, block, source in line_takes(m, t, step):

            @pl.when(valid)
            def _():
                line(way, step, chunk, block, source).wait_recv()

            if step + 1 < m - 1:
                go = valid & ((t < m - 1) if way == 0 else (t > 0))
                onward = t + 1 if way == 0 else t - 1

                @pl.when(go)
                def _():
                    line(way, step + 1, chunk, block, onward).start()

    stored = []
    for h in range(heads):
        if h % group == 0:
            finish(h // group)
        ctx_all[t, :, h * HD : (h + 1) * HD] = attend(h)
        send_line(0, h)
        out = pltpu.make_async_copy(
            ctx_all.at[t, :, pl.ds(h * HD, HD)],
            context.at[:, pl.ds(h * HD, HD)],
            local_sem.at[2 + h],
        )
        out.start()
        stored.append(out)
        advance(due[h])

    load.wait()

    def out_proj(block, first):
        for j in range(outs // wcols):
            cols = slice(j * wcols, (j + 1) * wcols)

            at = pl.multiple_of(block * wrows, 128)
            value = jnp.dot(
                ctx_all[block], w_all[pl.ds(at, wrows), cols], preferred_element_type=jnp.float32
            )
            acc[:, cols] = value + (residual[:, cols].astype(jnp.float32) if first else acc[:, cols])

    def add_blocks(step):
        def way(i, _):
            block = jnp.where(i == 0, t - 1 - step, t + 1 + step)

            @pl.when((block >= 0) & (block < m))
            def _():
                out_proj(block, False)

            return 0

        lax.fori_loop(0, 2, way, 0)

    for jobs in due[heads:]:
        advance(jobs)
    for d in range(m):
        finish(first_w + d)
    out_proj(t, True)
    for step in range(m - 1):
        if step == m - 2:
            for chunk in range(heads):
                take_line(step, chunk)
        add_blocks(step)

    residual[...] = acc[...].astype(jnp.bfloat16)
    final = pltpu.make_async_copy(residual, mixed, local_sem.at[1])
    final.start()

    for item in range(len(items)):
        drain(item)
    for f in order[1:]:

        @pl.when(far(f))
        def _():
            swap(f, False).wait_send()

    for step in range(m - 1):
        for cond, way, block, target in line_sends(m, t, step):
            for chunk in range(heads):

                @pl.when(cond)
                def _():
                    line(way, step, chunk, block, target).wait_send()

    for out in stored:
        out.wait()
    final.wait()


def attend_and_mix(n, m, q, kv, pos, tokens, w_out, w_mix, w_near):
    heads, rows, _ = q.shape
    kv_heads = kv.shape[0]
    wrows, wcols = w_out.shape
    outs = tokens.shape[1]
    items = kv_heads + 1 + m
    bf16, f32 = jnp.bfloat16, jnp.float32
    dma = pltpu.SemaphoreType.DMA
    return pl.pallas_call(
        functools.partial(attend_kernel, n, m),
        out_shape=(
            jax.ShapeDtypeStruct(tokens.shape, bf16),
            jax.ShapeDtypeStruct((rows, heads * HD), bf16),
        ),
        in_specs=[VMEM, VMEM, VMEM, ANY, ANY, ANY, ANY],
        out_specs=(ANY, ANY),
        scratch_shapes=[
            pltpu.VMEM((kv_heads, n * rows, 2 * HD), bf16),
            pltpu.VMEM((n, *pos.shape), pos.dtype),
            pltpu.VMEM((m, rows, heads * HD), bf16),
            pltpu.VMEM((m * wrows, outs), bf16),
            pltpu.VMEM((n, rows, rows), f32),
            pltpu.VMEM((rows, 128), f32),
            pltpu.VMEM((rows, HD), f32),
            pltpu.VMEM((rows, outs), f32),
            pltpu.VMEM((rows, outs), bf16),
            dma((items, plane_sems(n))),
            dma((items, plane_sems(n))),
            dma((m,)),
            dma((m,)),
            dma((2, m - 1, heads)),
            dma((2, m - 1, heads)),
            dma((2,)),
            dma((2 + heads,)),
        ],
        compiler_params=pltpu.CompilerParams(
            collective_id=1, has_side_effects=True, vmem_limit_bytes=60 * 2**20
        ),
        cost_estimate=pl.CostEstimate(flops=10**11, bytes_accessed=10**8, transcendentals=0),
    )(q, kv, pos, tokens, w_out, w_mix, w_near)


def shards(seq, tensor, tokens, positions, norm_gain, w_query, w_key, w_value, b_query, b_key, b_value, w_out):
    rows, feats = tokens.shape
    half = HD // 2
    inv_freq = ROPE_BASE ** (-jnp.arange(half, dtype=jnp.float32) * 2.0 / HD)
    inv_freq = jnp.concatenate((inv_freq, inv_freq))
    pos = jnp.broadcast_to(positions[None, :], (16, rows))
    q, kv, w_mix, w_near = project(
        seq, tensor, tokens, w_query, w_key, w_value, w_out,
        norm_gain.reshape(tensor, feats // w_query.shape[0], 1, w_query.shape[0]),
        b_query[None, :], b_key[None, :], b_value[None, :], positions[None, :], inv_freq[None, :],
    )
    return attend_and_mix(seq, tensor, q, kv, pos, tokens, w_out, w_mix, w_near)


def solution(mesh):
    in_specs = (
        P("seq", "tensor"),
        P("seq"),
        P(),
        P("seq", "tensor"),
        P("seq", "tensor"),
        P("seq", "tensor"),
        P("tensor"),
        P("tensor"),
        P("tensor"),
        P("tensor", "seq"),
    )
    out_specs = (P("seq", "tensor"), P("seq", "tensor"))

    def body(*args):
        return shards(mesh.shape["seq"], mesh.shape["tensor"], *args)

    return jax.shard_map(body, mesh=mesh, in_specs=in_specs, out_specs=out_specs, check_vma=False)
```
